32 devices in a mesh: seq: 8 (over y, x, core), tp: 4 (over z).
Axes of the slice: x: 2, y: 2, z: 4, core: 2. Of those that a mesh axis runs over, the one named last changes fastest.
Arguments:
- tokens: bfloat16 [4096, 3584], P('seq'), may hold values from -6 to 6
- norm_gain: float32 [3584], replicated, may hold values from 0.5 to 1.5
- q_weight: bfloat16 [3584, 3584], P(None, 'tp'), may hold values from -0.09375 to 0.09375
- q_bias: float32 [3584], P('tp'), may hold values from -9 to 9
- k_weight: bfloat16 [3584, 512], P(None, 'tp'), may hold values from -0.09375 to 0.09375
- k_bias: float32 [512], P('tp'), may hold values from -9 to 9
- v_weight: bfloat16 [3584, 512], P(None, 'tp'), may hold values from -0.09375 to 0.09375
- v_bias: float32 [512], P('tp'), may hold values from -5 to 5
- o_weight: bfloat16 [3584, 3584], P('tp'), may hold values from -0.09375 to 0.09375
- doc_ids: int32 [4096], replicated, may hold values from 0 to 7, never falling along the last dimension, each value on 1 to 2560 neighbouring positions
Outputs:
- attn_out: bfloat16 [4096, 3584], P('seq', 'tp')
The draws below stay inside these ranges and needn't reach their ends.
Inputs may be any that keep to these rules, and one draw needn't show every extreme that they name: `doc_ids`: document numbers never fall along the sequence; each document holds 1 to 2560 tokens and one holds exactly that many.
All inputs are finite; a program needn't handle non-finite values.
Results may differ from the reference program's by a relative error of at most 0.012.
Values may be sent and summed in bfloat16 or wider, within the bound.
No kernel may reach another device: no remote copies, remote signals or barrier semaphores. Data moves between devices by JAX's collectives and lax.ppermute only.
A program may use at most 128 MiB of HBM per device.

```python
import math
import jax
import jax.numpy as jnp
import numpy as np
from jax import lax

D = 3584
HQ = 28
KVH = 4
HD = 128
TOK_DEV = 512
DOCS = 8
TOKENS = 4096
N_TP = 4


def bias_noise(key, count):
    return jnp.clip(jax.random.normal(key, (count,), jnp.float32), -5.0, 5.0)


def bias_plan(key):
    base = jax.random.fold_in(key, 9157)
    signs = (jax.random.randint(jax.random.fold_in(base, 1), (HD,), 0, 2) * 2 - 1).astype(jnp.float32)
    across = jnp.arange(HD) % (HD // 2)
    pattern = jnp.where(across >= HD // 2 - HD // 8, signs, 0.0)
    strong = jax.random.randint(jax.random.fold_in(base, 2), (), 0, KVH)
    order = jax.random.permutation(jax.random.fold_in(base, 3), HQ // KVH)
    levels = [115.0, -105.0, 60.0, 30.0]
    tops = jnp.concatenate([jnp.array(levels, jnp.float32), jnp.zeros((HQ // KVH - 4,), jnp.float32)])
    strength = tops[order]
    key_level = math.sqrt(4.0 * levels[0] / math.sqrt(HD))
    return (pattern, strong, strength, key_level)


def draw_k_bias(key, part):
    pattern, strong, strength, key_level = bias_plan(key)
    noise = bias_noise(jax.random.fold_in(key, 31), KVH * HD).reshape(KVH, HD)
    chosen = (jnp.arange(KVH) == strong)[:, None] & (pattern != 0.0)[None, :]
    return jnp.where(chosen, key_level * pattern[None, :], noise).reshape(KVH * HD).astype(jnp.float32)


def draw_q_bias(key, part):
    pattern, strong, strength, key_level = bias_plan(key)
    group = HQ // KVH
    noise = bias_noise(jax.random.fold_in(key, 37), HQ * HD).reshape(KVH, group, HD)
    level = 4.0 * strength / (math.sqrt(HD) * key_level)
    chosen = (jnp.arange(KVH) == strong)[:, None, None] & (strength != 0.0)[None, :, None] & (pattern != 0.0)[None, None, :]
    aligned = level[None, :, None] * pattern[None, None, :]
    return jnp.where(chosen, aligned, noise).reshape(HQ * HD).astype(jnp.float32)


def shard_levels(stream_key, extent, split, smallest, top_value):
    gain = 1.0
    for dim, shards_of in split:
        draws = jax.random.uniform(jax.random.fold_in(jax.random.fold_in(stream_key, 6), dim), (shards_of,), jnp.float32, smallest / len(split), top_value / len(split))
        gain = gain * jnp.repeat(jnp.exp(draws), extent[dim] // shards_of).reshape((-1,) + (1,) * (len(extent) - 1 - dim))
    return gain


def length_profile(amount, total, most, skew):
    portions = [(1 << 20) // math.isqrt(standing ** skew) + 1 for standing in range(2, amount + 1)]
    rest, given = total - most - (amount - 1), [1] * (amount - 1)
    while rest > 0:
        movable = [i for i in range(amount - 1) if given[i] < most]
        pool, left = sum([portions[i] for i in movable]), rest
        for i in movable:
            addition = min(most - given[i], max(1, left * portions[i] // pool), rest)
            given[i] = given[i] + addition
            rest = rest - addition
    return np.array([most] + given)


def uneven_parts(stream_key, amount, total, most, lean):
    if amount == 2:
        one = jax.random.randint(stream_key, (), max(1, total - most), min(most, total - 1) + 1)
        return jnp.stack([one, total - one])
    lengths = jnp.asarray(length_profile(amount, total, most, lean), jnp.int32)
    twos = (amount - 1) // 2
    giver, taker = lengths[1:1 + 2 * twos:2], lengths[2:2 + 2 * twos:2]
    slack = jnp.minimum(giver - 1, most - taker)
    moved = jax.random.randint(jax.random.fold_in(stream_key, 1), (twos,), 0, 1 << 20) % (slack + 1)
    lengths = lengths.at[1:1 + 2 * twos:2].set(giver - moved).at[2:2 + 2 * twos:2].set(taker + moved)
    return lengths[jax.random.permutation(jax.random.fold_in(stream_key, 2), amount)]


def normal_values(own_key, shape, scale, reach, split=(), held_as=jnp.bfloat16):
    values = jax.random.normal(own_key, shape, jnp.float32) * scale
    if len(split) > 0:
        values = shard_levels(own_key, shape, split, -0.22, 0.18) * values
    return jnp.clip(values, min=-reach, max=reach).astype(held_as)


def setup_inputs(seed: int = 0) -> dict:
    key_list = jax.random.split(jax.random.key(seed), 11)
    tokens = normal_values(key_list[0], (TOKENS, D), 1.0, 6.0, ((0, 8),))
    norm_gain = jnp.clip(1.0 + 0.1 * jax.random.normal(key_list[1], (D,), jnp.float32), 0.5, 1.5)
    q_weight = normal_values(key_list[2], (D, HQ * HD), D ** -0.5, 0.09375, ((1, 4),))
    q_bias = draw_q_bias(jax.random.fold_in(key_list[10], 71), 0)
    k_weight = normal_values(key_list[4], (D, KVH * HD), D ** -0.5, 0.09375, ((1, 4),))
    k_bias = draw_k_bias(jax.random.fold_in(key_list[10], 71), 0)
    v_weight = normal_values(key_list[6], (D, KVH * HD), D ** -0.5, 0.09375, ((1, 4),))
    v_bias = normal_values(key_list[7], (KVH * HD,), 1.0, 5.0, ((0, 4),), jnp.float32)
    o_weight = normal_values(key_list[8], (HQ * HD, D), (HQ * HD) ** -0.5, 0.09375, ((0, 4),))
    doc_ids = jnp.searchsorted(jnp.cumsum(uneven_parts(key_list[9], DOCS, TOKENS, TOKENS // 2 + TOK_DEV, 0)), jnp.arange(TOKENS), side="right").astype(jnp.int32)
    return {"tokens": tokens, "norm_gain": norm_gain, "q_weight": q_weight, "q_bias": q_bias, "k_weight": k_weight, "k_bias": k_bias, "v_weight": v_weight, "v_bias": v_bias, "o_weight": o_weight, "doc_ids": doc_ids}


rope_base = 1000000.0

def rotate(t, posf):
    half = t.shape[-1] // 2
    inv = rope_base ** (-(jnp.arange(half, dtype=jnp.float32) * 2.0) / t.shape[-1])
    angle = posf[:, None] * inv[None, :]
    angle = jnp.concatenate([angle, angle], axis=-1)
    turned = jnp.concatenate([-t[..., half:], t[..., :half]], axis=-1)
    return t * jnp.cos(angle)[:, None, :] + turned * jnp.sin(angle)[:, None, :]

def reference(tokens, norm_gain, q_weight, q_bias, k_weight, k_bias, v_weight, v_bias, o_weight, doc_ids):
    widened = tokens.astype(jnp.float32)
    normed = (widened * lax.rsqrt(lax.optimization_barrier(jnp.mean(widened * widened, axis=-1, keepdims=True)) + 1e-06) * norm_gain).astype(jnp.bfloat16)
    posf = jnp.arange(TOKENS).astype(jnp.float32)
    group = HQ // KVH
    query = jnp.dot(normed, q_weight, preferred_element_type=jnp.float32) + q_bias
    query = rotate(query.reshape(TOKENS, HQ, HD), posf).astype(jnp.bfloat16).reshape(TOKENS, KVH, group, HD)
    keys = jnp.dot(normed, k_weight, preferred_element_type=jnp.float32) + k_bias
    keys = rotate(keys.reshape(TOKENS, KVH, HD), posf).astype(jnp.bfloat16)
    values = (jnp.dot(normed, v_weight, preferred_element_type=jnp.float32) + v_bias).astype(jnp.bfloat16).reshape(TOKENS, KVH, HD)
    block = min(512, TOKENS)
    scale = 1.0 / HD ** 0.5
    kpos = jnp.arange(TOKENS).astype(jnp.int32)
    keys_f = keys.astype(jnp.float32)
    values_f = values.astype(jnp.float32)

    def attend(index):
        first = (index * block).astype(jnp.int32)
        qblock = lax.dynamic_slice_in_dim(query, first, block, 0).astype(jnp.float32)
        qdoc = lax.dynamic_slice_in_dim(doc_ids, first, block, 0)
        qpos = first + jnp.arange(block).astype(jnp.int32)
        scores = jnp.einsum('qkgd,tkd->kgqt', qblock, keys_f) * scale
        visible = (kpos[None, :] <= qpos[:, None]) & (qdoc[:, None] == doc_ids[None, :])
        scores = jnp.where(visible, scores, -1e+30)
        top = lax.optimization_barrier(jnp.max(scores, axis=-1, keepdims=True))
        expd = jnp.where(visible, jnp.exp(scores - top), 0.0)
        total = lax.optimization_barrier(jnp.sum(expd, axis=-1))
        weights = expd.astype(jnp.bfloat16).astype(jnp.float32)
        summed = jnp.einsum('kgqt,tkd->kgqd', weights, values_f) / total[..., None]
        return jnp.transpose(summed, (2, 0, 1, 3)).astype(jnp.bfloat16).reshape(block, HQ * HD)
    context = lax.map(attend, jnp.arange(TOKENS // block)).reshape(TOKENS, HQ * HD)
    width = HQ * HD // N_TP
    result = jnp.zeros((TOKENS, D), jnp.float32)
    for index in range(N_TP):
        term = jnp.dot(context[:, index * width:(index + 1) * width], o_weight[index * width:(index + 1) * width], preferred_element_type=jnp.float32)
        result = result + term.astype(jnp.bfloat16).astype(jnp.float32)
    return result.astype(jnp.bfloat16)
```

```python
import functools
import math

import jax
import jax.numpy as jnp
import numpy as np
from jax import lax
from jax.experimental import pallas as pl
from jax.experimental.pallas import tpu as pltpu
from jax.sharding import PartitionSpec as P

HD = 128
EPS = 1e-06
TILE = 128
ROPE_BASE = 1000000.0
NEG = -1e30


def cost(flops, moved, exps=0):
    return pl.CostEstimate(flops=flops, bytes_accessed=moved, transcendentals=exps)


def rope_tables(rows, count):
    inv = ROPE_BASE ** (-(np.arange(HD // 2, dtype=np.float64) * 2.0) / HD)
    inv = np.concatenate([inv, inv])
    near = np.arange(rows)[:, None] * inv[None, :]
    far = (np.arange(count) * rows)[:, None] * inv[None, :]

    def held(table):
        return jnp.asarray(table.astype(np.float32))

    return held(np.cos(far)), held(np.sin(far)), held(np.cos(near)), held(np.sin(near))


def turn(t, cos, sin):
    return t * cos + pltpu.roll(t, HD // 2, 1) * sin


VMEM = 67043328


def params(mib=None):
    return pltpu.CompilerParams(vmem_limit_bytes=VMEM if mib is None else mib << 20)


def angles(fcos_ref, fsin_ref, ncos, nsin):
    at = pl.ds(lax.axis_index("seq"), 1)
    fcos, fsin = fcos_ref[at, :], fsin_ref[at, :]
    cos = fcos * ncos - fsin * nsin
    sin = fsin * ncos + fcos * nsin
    lane = lax.broadcasted_iota(jnp.int32, cos.shape, 1)
    return cos, jnp.where(lane < HD // 2, -sin, sin)


def gained(x_s, gain_ref, at):
    x = x_s[:, at].astype(jnp.float32)
    return x, (x * gain_ref[at][None, :]).astype(jnp.bfloat16)


def norm_kv_kernel(
    depth,
    x_ref, gain_ref, wk_ref, bk_ref, wv_ref, bv_ref, fcos_ref, fsin_ref, ncos_ref, nsin_ref,
    kv_ref, r_ref, x_s, wk_s, wv_s, cos_s, sin_s, k_s, v_s, sq_s, sem,
):
    width = x_s.shape[1]
    steps = width // depth

    def copies(c):
        at = pl.ds(pl.multiple_of(c * depth, depth), depth)
        return [
            pltpu.make_async_copy(x_ref.at[:, at], x_s.at[:, at], sem.at[0, c]),
            pltpu.make_async_copy(wk_ref.at[at], wk_s.at[at], sem.at[1, c]),
            pltpu.make_async_copy(wv_ref.at[at], wv_s.at[at], sem.at[2, c]),
        ]

    tables = [
        pltpu.make_async_copy(ncos_ref, cos_s, sem.at[0, steps]),
        pltpu.make_async_copy(nsin_ref, sin_s, sem.at[1, steps]),
    ]
    for c in range(steps):
        for copy in copies(c):
            copy.start()
    for copy in tables:
        copy.start()
    for ref in (k_s, v_s, sq_s):
        ref[...] = jnp.zeros_like(ref)

    def one(c, carry):
        for copy in copies(c):
            copy.wait()
        at = pl.ds(pl.multiple_of(c * depth, depth), depth)
        x, y = gained(x_s, gain_ref, at)
        sq = x * x
        sq_s[...] += sum(sq[:, i * HD:(i + 1) * HD] for i in range(depth // HD))
        k_s[...] += jnp.dot(y, wk_s[at, :], preferred_element_type=jnp.float32)
        v_s[...] += jnp.dot(y, wv_s[at, :], preferred_element_type=jnp.float32)
        return carry

    lax.fori_loop(0, steps, one, 0)
    for copy in tables:
        copy.wait()
    mean = jnp.sum(sq_s[...], axis=-1, keepdims=True) / width
    r = jnp.broadcast_to(lax.rsqrt(mean + EPS), sq_s.shape)
    r_ref[...] = r
    cos, sin = angles(fcos_ref, fsin_ref, cos_s[...], sin_s[...])
    kv_ref[0] = turn(k_s[...] * r + bk_ref[...][None, :], cos, sin).astype(jnp.bfloat16)
    kv_ref[1] = (v_s[...] * r + bv_ref[...][None, :]).astype(jnp.bfloat16)


ANYWHERE = pl.BlockSpec(memory_space=pl.ANY)
HERE = pl.BlockSpec(memory_space=pltpu.VMEM)


def norm_kv(tokens, gain, wk, bk, wv, bv, tables):
    rows, width = tokens.shape
    depth = math.gcd(512, width)
    return pl.pallas_call(
        functools.partial(norm_kv_kernel, depth),
        in_specs=[ANYWHERE, HERE, ANYWHERE, HERE, ANYWHERE, HERE, HERE, HERE, ANYWHERE, ANYWHERE],
        out_specs=[HERE, HERE],
        out_shape=[
            jax.ShapeDtypeStruct((2, rows, HD), jnp.bfloat16),
            jax.ShapeDtypeStruct((rows, HD), jnp.float32),
        ],
        scratch_shapes=[
            pltpu.VMEM((rows, width), jnp.bfloat16),
            pltpu.VMEM((width, HD), jnp.bfloat16),
            pltpu.VMEM((width, HD), jnp.bfloat16),
            *[pltpu.VMEM((rows, HD), jnp.float32)] * 5,
            pltpu.SemaphoreType.DMA((3, width // depth + 1)),
        ],
        cost_estimate=cost(4 * rows * width * HD, 2 * rows * width + 4 * width * HD),
        compiler_params=params(),
        name="norm_kv",
    )(tokens, gain, wk, bk, wv, bv, *tables)


def query_kernel(
    depth, heads,
    x_ref, gain_ref, w_ref, b_ref, r_ref, fcos_ref, fsin_ref, ncos_ref, nsin_ref,
    o_ref, x_s, w_s, r_s, cos_s, sin_s, acc_s, sem,
):
    steps = x_s.shape[1] // depth

    def copies(c):
        at = pl.ds(pl.multiple_of(c * depth, depth), depth)
        return [
            pltpu.make_async_copy(x_ref.at[:, at], x_s.at[:, at], sem.at[0, c]),
            pltpu.make_async_copy(w_ref.at[at], w_s.at[at], sem.at[1, c]),
        ]

    tables = [
        pltpu.make_async_copy(ncos_ref, cos_s, sem.at[0, steps]),
        pltpu.make_async_copy(nsin_ref, sin_s, sem.at[1, steps]),
        pltpu.make_async_copy(r_ref, r_s, sem.at[2, 0]),
    ]
    for c in range(steps):
        for copy in copies(c):
            copy.start()
    for copy in tables:
        copy.start()
    acc_s[...] = jnp.zeros_like(acc_s)

    def one(c, carry):
        for copy in copies(c):
            copy.wait()
        at = pl.ds(pl.multiple_of(c * depth, depth), depth)
        y = gained(x_s, gain_ref, at)[1]
        acc_s[...] += jnp.dot(y, w_s[at, :], preferred_element_type=jnp.float32)
        return carry

    lax.fori_loop(0, steps, one, 0)
    for copy in tables:
        copy.wait()
    scale = math.log2(math.e) / math.sqrt(HD)
    cos, sin = angles(fcos_ref, fsin_ref, cos_s[...] * scale, sin_s[...] * scale)
    r = r_s[...]
    for h in range(heads):
        at = slice(h * HD, (h + 1) * HD)
        t = turn(acc_s[:, at] * r + b_ref[at][None, :], cos, sin).astype(jnp.bfloat16)
        for i in range(t.shape[0] // TILE):
            o_ref[i, h] = t[i * TILE:(i + 1) * TILE]


def queries(tokens, gain, wq, bq, r, tables):
    rows, width = tokens.shape
    cols = wq.shape[1]
    heads = cols // HD
    depth = math.gcd(512, width)
    return pl.pallas_call(
        functools.partial(query_kernel, depth, heads),
        in_specs=[ANYWHERE, HERE, ANYWHERE, HERE, ANYWHERE, HERE, HERE, ANYWHERE, ANYWHERE],
        out_specs=HERE,
        out_shape=jax.ShapeDtypeStruct((rows // TILE, heads, TILE, HD), jnp.bfloat16),
        scratch_shapes=[
            pltpu.VMEM((rows, width), jnp.bfloat16),
            pltpu.VMEM((width, cols), jnp.bfloat16),
            *[pltpu.VMEM((rows, HD), jnp.float32)] * 3,
            pltpu.VMEM((rows, cols), jnp.float32),
            pltpu.SemaphoreType.DMA((3, width // depth + 1)),
        ],
        cost_estimate=cost(2 * rows * width * cols, 2 * rows * width + 2 * width * cols),
        compiler_params=params(),
        name="queries",
    )(tokens, gain, wq, bq, r, *tables)


GROUPS = 1
KT = 512


def split_heads(heads):
    parts = min(GROUPS, heads)
    return [heads // parts + (i < heads % parts) for i in range(parts)]


def attend_kernel(
    reach, heads, rows, first, kt,
    bounds_ref, q_ref, qdoc_ref, kdoc_ref, mine_ref, other_ref,
    o_ref, k_s, v_s, m_s, l_s, acc_s, sem,
):
    step = pl.program_id(0)
    odd = bounds_ref[0, 0]

    @pl.when(step == 0)
    def _():
        copies = []
        for d in range(reach + 1):
            if d % 2 == 0:
                source = mine_ref.at[d // 2]
            else:
                source = other_ref.at[(d - 1) // 2 + 1 - odd]
            at = pl.ds((reach - d) * rows, rows)
            copies.append(pltpu.make_async_copy(source.at[0], k_s.at[at], sem.at[2 * d]))
            copies.append(pltpu.make_async_copy(source.at[1], v_s.at[at], sem.at[2 * d + 1]))
        for c in copies:
            c.start()
        for c in copies:
            c.wait()

    total = heads * TILE
    m_s[...] = jnp.full((total, HD), NEG, jnp.float32)
    l_s[...] = jnp.zeros((total, HD), jnp.float32)
    acc_s[...] = jnp.zeros((total, HD), jnp.float32)

    tile = step + first
    low, edge = bounds_ref[1, tile], bounds_ref[2, tile]
    q0 = reach * rows + tile * TILE
    q = q_ref[0].reshape(total, HD)

    def chunk(c, masked):
        start = pl.multiple_of(c * kt, kt)
        k = k_s[pl.ds(start, kt), :]
        v = v_s[pl.ds(start, kt), :]
        if masked:
            kpos = start + lax.broadcasted_iota(jnp.int32, (TILE, kt), 1)
            qpos = q0 + lax.broadcasted_iota(jnp.int32, (TILE, kt), 0)
            seen = (kpos <= qpos) & (kdoc_ref[:, pl.ds(start, kt)] == qdoc_ref[...])
            bias = jnp.where(seen, 0.0, NEG)

        def score(at):
            return lax.dot_general(q[at], k, (((1,), (1,)), ((), ())), preferred_element_type=jnp.float32)

        groups = []
        begin = 0
        for size in split_heads(heads):
            groups.append(slice(begin * TILE, (begin + size) * TILE))
            begin += size
        scores = [score(groups[0])]
        for i, at in enumerate(groups):
            if i + 1 < len(groups):
                scores.append(score(groups[i + 1]))
            s = scores[i]
            if masked:
                s = (s.reshape(-1, TILE, kt) + bias[None]).reshape(-1, kt)
            old = m_s[at]
            new = jnp.maximum(old, jnp.max(s, axis=-1, keepdims=True))
            p = jnp.exp2(s - jnp.concatenate([new] * (kt // HD), axis=1))
            alpha = jnp.exp2(old - new)
            m_s[at] = new
            l_s[at] = l_s[at] * alpha + sum(p[:, i * HD:(i + 1) * HD] for i in range(kt // HD))
            acc_s[at] = acc_s[at] * alpha + jnp.dot(p.astype(jnp.bfloat16), v, preferred_element_type=jnp.float32)

    def one(c, carry):
        partial = (c * kt < edge) | ((c + 1) * kt > q0 + 1)

        @pl.when(partial)
        def _():
            chunk(c, True)

        @pl.when(jnp.logical_not(partial))
        def _():
            chunk(c, False)

        return carry

    lax.fori_loop(low // kt, (q0 + TILE - 1) // kt + 1, one, 0)
    out = acc_s[...] / jnp.sum(l_s[...], axis=-1, keepdims=True)
    for h in range(heads):
        o_ref[:, h * HD:(h + 1) * HD] = out[h * TILE:(h + 1) * TILE].astype(jnp.bfloat16)


def attend(bounds, q, qdoc, kdoc, mine, other, reach, rows, first, tiles):
    heads = q.shape[1]
    cols = heads * HD
    kt = math.gcd(KT, rows)
    window = (reach + 1) * rows
    work = tiles * TILE * heads * (reach + 1) * rows
    return pl.pallas_call(
        functools.partial(attend_kernel, reach, heads, rows, first, kt),
        grid=(tiles,),
        in_specs=[
            pl.BlockSpec(memory_space=pltpu.SMEM),
            pl.BlockSpec((1, heads, TILE, HD), lambda i: (i + first, 0, 0, 0)),
            pl.BlockSpec((TILE, 1), lambda i: (i + first, 0)),
            pl.BlockSpec((1, window), lambda i: (0, 0)),
            pl.BlockSpec(memory_space=pl.ANY),
            pl.BlockSpec(memory_space=pl.ANY),
        ],
        out_specs=pl.BlockSpec((TILE, cols), lambda i: (i, 0)),
        out_shape=jax.ShapeDtypeStruct((tiles * TILE, cols), jnp.bfloat16),
        scratch_shapes=[
            pltpu.VMEM((window, HD), jnp.bfloat16),
            pltpu.VMEM((window, HD), jnp.bfloat16),
            pltpu.VMEM((heads * TILE, HD), jnp.float32),
            pltpu.VMEM((heads * TILE, HD), jnp.float32),
            pltpu.VMEM((heads * TILE, HD), jnp.float32),
            pltpu.SemaphoreType.DMA((2 * (reach + 1),)),
        ],
        cost_estimate=cost(4 * work * HD, 2 * tiles * TILE * cols, work),
        compiler_params=params(28),
        name=f"attend_{first}",
    )(bounds, q, qdoc, kdoc, mine, other)


def terms_kernel(c_ref, w_ref, o_ref):
    o_ref[0] = jnp.dot(c_ref[...], w_ref[...], preferred_element_type=jnp.float32).astype(jnp.bfloat16)


def group_terms(context, weight, parts):
    rows, depth = context.shape
    cols = weight.shape[1] // parts
    return pl.pallas_call(
        terms_kernel,
        grid=(parts,),
        in_specs=[
            pl.BlockSpec((rows, depth), lambda i: (0, 0)),
            pl.BlockSpec((depth, cols), lambda i: (0, i)),
        ],
        out_specs=pl.BlockSpec((1, rows, cols), lambda i: (i, 0, 0)),
        out_shape=jax.ShapeDtypeStruct((parts, rows, cols), jnp.bfloat16),
        cost_estimate=cost(2 * rows * depth * cols * parts, 2 * depth * cols * parts),
        compiler_params=params(16),
        name="group_terms",
    )(context, weight)


def wide(t):
    return t.astype(jnp.float32)


def both_ways(value_right, value_left, axis, count):
    ahead = [(i, i + 1) for i in range(count - 1)]
    back = [(j, i) for i, j in ahead]
    return lax.ppermute(value_right, axis, ahead), lax.ppermute(value_left, axis, back)


def spread_weight(o_weight, parts, pieces, place, me):
    depth, width = o_weight.shape
    cols, piece = width // parts, depth // pieces
    row = (place % pieces) * piece
    got = []
    for r in range(1, parts):
        target = lax.rem(me + r, parts)
        block = lax.dynamic_slice(o_weight, (row, target * cols), (piece, cols))
        got.append(lax.ppermute(block, "tp", [(i, (i + r) % parts) for i in range(parts)]))
    return got


def swap(value, bit, count):
    return lax.ppermute(value, "seq", [(i, i ^ (1 << bit)) for i in range(count)])


def final_kernel(
    parts, pieces, cuts, orders,
    c_ref, *refs,
):
    hops = refs[:2 * (parts - 1)]
    w_ref, kept0, got0, kept1, got1 = refs[2 * (parts - 1):2 * (parts - 1) + 5]
    o_ref, c_s, w_s, acc_s, csem, wsem = refs[2 * (parts - 1) + 5:]
    me = lax.axis_index("tp")
    spot = lax.rem(lax.axis_index("seq"), pieces)
    depth, cols = w_s.shape[1:]
    piece = depth // pieces

    own = pltpu.make_async_copy(w_ref.at[:, pl.ds(pl.multiple_of(me * cols, cols), cols)], w_s.at[0], wsem.at[0])
    mine = pltpu.make_async_copy(c_ref, c_s.at[0], csem.at[0])
    own.start()
    mine.start()
    copies = []
    for r in range(1, parts):
        now = []
        for half, (kept, got) in enumerate(((kept0, got0), (kept1, got1))):
            low, size = cuts[half]
            steps = len(orders[half])
            for j in range(pieces):
                mask = sum(((j >> s) & 1) << orders[half][s] for s in range(steps))
                source = kept if j < pieces // 2 else got
                p = spot ^ mask
                at = pl.ds(pl.multiple_of(p * piece + low, 16 if piece % 16 == 0 else 1), size)
                now.append(pltpu.make_async_copy(source.at[j % (pieces // 2), r - 1], w_s.at[r, at], wsem.at[1 + len(copies) * 2 * pieces + len(now)]))
        for c in now:
            c.start()
        copies.append(now)

    def context(r, go):
        for k in range(1, parts):
            if k == r:
                @pl.when(me >= r)
                def _():
                    go(pltpu.make_async_copy(hops[2 * (k - 1)], c_s.at[r], csem.at[r]))

            if k == parts - r:
                @pl.when(me < r)
                def _():
                    go(pltpu.make_async_copy(hops[2 * (k - 1) + 1], c_s.at[r], csem.at[r]))

    for r in range(1, parts):
        context(r, lambda c: c.start())
    own.wait()
    mine.wait()
    acc_s[...] = jnp.dot(c_s[0], w_s[0], preferred_element_type=jnp.float32)
    for r in range(1, parts):
        context(r, lambda c: c.wait())
        for c in copies[r - 1]:
            c.wait()
        acc_s[...] += jnp.dot(c_s[r], w_s[r], preferred_element_type=jnp.float32)
    o_ref[...] = acc_s[...].astype(jnp.bfloat16)


def final(context, hops, o_weight, shares, parts, pieces, cuts, orders):
    rows, depth = context.shape
    cols = o_weight.shape[1] // parts
    anywhere = pl.BlockSpec(memory_space=pl.ANY)
    operands = [context, *hops, o_weight, *shares]
    return pl.pallas_call(
        functools.partial(final_kernel, parts, pieces, cuts, orders),
        grid=(1,),
        in_specs=[anywhere] * len(operands),
        out_specs=pl.BlockSpec((rows, cols), lambda i: (0, 0)),
        out_shape=jax.ShapeDtypeStruct((2 * rows, cols), jnp.bfloat16),
        scratch_shapes=[
            pltpu.VMEM((parts, rows, depth), jnp.bfloat16),
            pltpu.VMEM((parts, depth, cols), jnp.bfloat16),
            pltpu.VMEM((rows, cols), jnp.float32),
            pltpu.SemaphoreType.DMA((parts,)),
            pltpu.SemaphoreType.DMA((1 + 2 * pieces * (parts - 1),)),
        ],
        cost_estimate=cost(2 * rows * depth * parts * cols, 2 * parts * depth * cols),
        compiler_params=params(24),
        name="final",
    )(*operands)


def join_kernel(own_ref, right_ref, left_ref, held_ref, o_ref):
    total = wide(own_ref[...][0]) + wide(right_ref[...]) + wide(left_ref[...])
    o_ref[...] = total.astype(jnp.bfloat16)


def join(own, right, left, held):
    rows, cols = right.shape
    tiled = pl.BlockSpec((rows, cols), lambda i: (i, 0))
    return pl.pallas_call(
        join_kernel,
        grid=(1,),
        in_specs=[
            pl.BlockSpec((1, rows, cols), lambda i: (lax.axis_index("tp"), 0, 0)),
            tiled,
            tiled,
            pl.BlockSpec(memory_space=pl.ANY),
        ],
        out_specs=pl.BlockSpec((rows, cols), lambda i: (1, 0)),
        out_shape=jax.ShapeDtypeStruct(held.shape, jnp.bfloat16),
        input_output_aliases={3: 0},
        cost_estimate=cost(2 * rows * cols, 8 * rows * cols),
        compiler_params=params(16),
        name="join",
    )(own, right, left, held)


def body(tokens, norm_gain, q_weight, q_bias, k_weight, k_bias, v_weight, v_bias, o_weight, doc_ids):
    rows = tokens.shape[0]
    count = lax.axis_size("seq")
    parts = lax.axis_size("tp")
    place = lax.axis_index("seq")
    first_row = place * rows
    reach = (count * rows // 2 + 2 * rows - 2) // rows
    reach = min(reach, count - 1)
    tables = rope_tables(rows, count)
    kv, r = norm_kv(tokens, norm_gain, k_weight, k_bias, v_weight, v_bias, tables)

    got = [kv]
    for s in range(1, (reach + 1) // 2 + 1):
        pairs = [(i, i + 2 * s) for i in range(count - 2 * s)]
        if 2 * s > reach:
            pairs = [(i, j) for i, j in pairs if i % 2 == 1]
        got.append(lax.ppermute(kv, "seq", pairs))
    me = lax.axis_index("tp")
    pieces = min(count, 8)
    piece = o_weight.shape[0] // pieces
    low = (piece // 2 + 15) // 16 * 16
    cuts = [(0, low), (low, piece - low)]
    bits = pieces.bit_length() - 1
    orders = [list(range(bits - 1, -1, -1)), [*range(1, bits), 0]]
    share = spread_weight(o_weight, parts, pieces, place, me)

    query = queries(tokens, norm_gain, q_weight, q_bias, r, tables)
    query, got = lax.optimization_barrier((query, got))
    mine = jnp.stack(got)
    other = lax.ppermute(mine, "seq", [(i, i ^ 1) for i in range(count)])

    kdoc = lax.dynamic_slice_in_dim(
        jnp.pad(doc_ids, (reach * rows, 0), constant_values=-1), first_row, (reach + 1) * rows, 0
    )
    qdoc = kdoc[reach * rows:]
    tiles = rows // TILE
    ends = qdoc.reshape(tiles, TILE)[:, jnp.array([0, TILE - 1])]
    starts = jnp.sum((doc_ids[None, None, :] < ends[:, :, None]).astype(jnp.int32), axis=-1)
    starts = jnp.maximum(starts - (first_row - reach * rows), 0).T
    odd = jnp.full((1, tiles), place % 2, jnp.int32)
    bounds = jnp.concatenate([odd, starts.astype(jnp.int32)], axis=0)

    def attended(first, tiles):
        return attend(bounds, query, qdoc[:, None], kdoc[None, :], mine, other, reach, rows, first, tiles)

    ahead = attended(0, tiles // 2)
    right, left = both_ways(ahead, ahead, "tp", parts)
    hops = [right, left]
    share = jnp.stack(lax.optimization_barrier((share, ahead))[0])
    shares = []
    for (low, size), order in zip(cuts, orders):
        held = share[:, low:low + size][None]
        for bit in order[:-1]:
            held = jnp.concatenate([held, swap(held, bit, count)], axis=0)
        shares += [held, swap(held, order[-1], count)]

    terms = group_terms(attended(tiles // 2, tiles - tiles // 2), o_weight, parts)
    last = parts - 1

    def term(d):
        return wide(lax.dynamic_index_in_dim(terms, jnp.clip(d, 0, last), 0, False))

    for slot in range(2, parts + 1):
        to_right = wide(right) + jnp.where(me >= slot - 1, 0.0, term(me + parts + 1 - slot))
        to_left = wide(left) + jnp.where(last - me >= slot - 1, 0.0, term(me - parts - 1 + slot))
        right, left = both_ways(to_right.astype(jnp.bfloat16), to_left.astype(jnp.bfloat16), "tp", parts)
        if slot < parts:
            hops += [right, left]
    done = final(ahead, hops, o_weight, shares, parts, pieces, cuts, orders)
    return join(terms, right, left, done)


def solution(mesh):
    placed = (
        P("seq", None),
        P(),
        P(None, "tp"),
        P("tp"),
        P(None, "tp"),
        P("tp"),
        P(None, "tp"),
        P("tp"),
        P("tp", None),
        P(),
    )
    return jax.shard_map(
        body, mesh=mesh, in_specs=placed, out_specs=P("seq", "tp"), check_vma=False
    )
```
